256 devices in a mesh: expert: 64 (over x, z, core), dp: 4 (over y).
Axes of the slice: x: 4, y: 4, z: 8, core: 2. Of those that a mesh axis runs over, the one named last changes fastest.
Arguments:
- tokens: bfloat16 [65536, 2048], P(('expert', 'dp')), may hold values from -256 to 256
- routes: int32 [65536, 2], P(('expert', 'dp')), may hold values from 0 to 255, all different within a row
- priority: int32 [256, 256], P(('expert', 'dp')), may hold values from 0 to 255, each once within a row
- router: bfloat16 [2048, 256], replicated, may hold values from -3 to 3
- w_in: bfloat16 [256, 2048, 1024], P(('expert', 'dp')), may hold values from -0.125 to 0.125
- w_out: bfloat16 [256, 2048, 1024], P(('expert', 'dp')), may hold values from -0.1875 to 0.1875
Outputs:
- mixed: bfloat16 [65536, 2048], P(('expert', 'dp'))
- aux_loss: float32 [], replicated
The draws below stay inside these ranges and needn't reach their ends.
Inputs may be any that keep to these rules, and one draw needn't show every extreme that they name: `routes`: a token's two experts differ; every expert is named by some token. `priority`: each group's 256 tokens hold every rank once.
All inputs are finite; a program needn't handle non-finite values.
Results may differ from the reference program's by a relative error of at most 0.0014.
The reference program's roundings to bfloat16 on the way count: a program that leaves them out, or rounds other values in their place, can miss the bound.
Values may be sent and summed in bfloat16 or wider, within the bound.
No kernel may reach another device: no remote copies, remote signals or barrier semaphores. Data moves between devices by JAX's collectives and lax.ppermute only.
A program may use at most 64 MiB of HBM per device.

```python
import math
import jax
import jax.numpy as jnp
from jax import lax

D = 2048
FF = 1024
TOK_DEV = 256
EXPERTS = 256
GROUPS = 256
TOKENS = 65536
CAP = 4


def router_values(key):
    sub_key = jax.random.fold_in(key, 71)
    spread = 3.0 / math.sqrt(D)
    values = jnp.clip(jax.random.normal(sub_key, (D, EXPERTS), jnp.float32), -6.0, 6.0) * spread
    return values


def draw_router(key, part):
    return router_values(key).astype(jnp.bfloat16)


def draw_tokens(key, part):
    base = jnp.clip(jax.random.normal(jax.random.fold_in(key, 5), (TOKENS, D), jnp.float32), -6.0, 6.0)
    return base.astype(jnp.bfloat16)


def block_scale(own_key, dims, cuts, low, top_value):
    gain, own = 1.0, jax.random.fold_in(own_key, 6)
    for position, parts in cuts:
        draws = jnp.exp(jax.random.uniform(jax.random.fold_in(own, position), (parts,), jnp.float32, low / len(cuts), top_value / len(cuts)))
        gain = gain * jnp.repeat(draws, dims[position] // parts).reshape([-1 if axis == position else 1 for axis in range(len(dims))])
    return gain


def distinct(rng, rows, count, top, lift):
    sequence = jax.random.permutation(jax.random.fold_in(rng, 1), count)
    favour = sequence
    for power in range(3):
        favour = favour * favour // count
    favour = favour * lift // count
    chance = jax.random.randint(jax.random.fold_in(rng, 2), (rows, count), 0, 4096) + favour
    fixed_rows = jax.random.permutation(jax.random.fold_in(rng, 3), rows)[jnp.arange(count) % rows]
    chance = jnp.where(jnp.arange(rows)[:, None] == fixed_rows[None, :], 1 << 14, chance)
    score = chance * count + jnp.arange(count)
    return lax.top_k(score.astype(jnp.int32), top)[1].astype(jnp.int32)


def noise(key, dims, width, bound, pieces=(), kind=jnp.bfloat16):
    level = block_scale(key, dims, pieces, -0.22, 0.18) if pieces else 1.0
    entries = jax.random.normal(key, dims, jnp.float32) * width * level
    return jnp.minimum(jnp.maximum(entries, -bound), bound).astype(kind)


def setup_inputs(seed: int = 0) -> dict:
    arg_keys = jax.random.split(jax.random.key(seed), 7)
    return {
        "tokens": draw_tokens(jax.random.fold_in(arg_keys[6], 71), 0),
        "routes": distinct(arg_keys[1], TOKENS, EXPERTS, 2, 64),
        "priority": jax.vmap(lambda own: jax.random.permutation(own, TOK_DEV))(jax.random.split(arg_keys[2], GROUPS)).reshape((GROUPS, TOK_DEV)).astype(jnp.int32),
        "router": draw_router(jax.random.fold_in(arg_keys[6], 71), 0),
        "w_in": noise(arg_keys[4], (EXPERTS, D, FF), D ** -0.5, 0.125, ((0, 256),)),
        "w_out": noise(arg_keys[5], (EXPERTS, D, FF), FF ** -0.5, 0.1875, ((0, 256),)),
    }


def reference(tokens, routes, priority, router, w_in, w_out):
    group_count = TOKENS // TOK_DEV
    logits = jnp.dot(tokens, router, preferred_element_type=jnp.float32)
    probs = jax.nn.softmax(logits, axis=-1)
    first = routes[:, 0].astype(jnp.int32)
    second = routes[:, 1].astype(jnp.int32)
    logit_first = jnp.take_along_axis(logits, first[:, None], axis=1)[:, 0]
    logit_second = jnp.take_along_axis(logits, second[:, None], axis=1)[:, 0]
    gate_first = jax.nn.sigmoid(logit_first - logit_second).astype(jnp.bfloat16)
    gate_second = jax.nn.sigmoid(logit_second - logit_first).astype(jnp.bfloat16)
    expert_ids = jnp.arange(EXPERTS, dtype=jnp.int32)
    first_grouped = first.reshape(group_count, TOK_DEV)
    second_grouped = second.reshape(group_count, TOK_DEV)

    def positions(items):
        first_row, second_row, ranks = items
        first_hot = (first_row[:, None] == expert_ids[None, :]).astype(jnp.float32)
        second_hot = (second_row[:, None] == expert_ids[None, :]).astype(jnp.float32)
        earlier = (ranks[None, :] < ranks[:, None]).astype(jnp.float32)
        before_first = jnp.dot(earlier, first_hot, preferred_element_type=jnp.float32)
        before_second = jnp.dot(earlier, second_hot, preferred_element_type=jnp.float32)
        first_load = jnp.sum(first_hot, axis=0)
        pos_first = jnp.sum(before_first * first_hot, axis=1)
        pos_second = jnp.sum((before_second + first_load[None, :]) * second_hot, axis=1)
        return pos_first.astype(jnp.int32), pos_second.astype(jnp.int32)

    pos_first, pos_second = lax.map(positions, (first_grouped, second_grouped, priority))
    dump_slot = CAP * EXPERTS
    slot_first = jnp.where(pos_first < CAP, pos_first * EXPERTS + first_grouped, dump_slot).astype(jnp.int32)
    slot_second = jnp.where(pos_second < CAP, pos_second * EXPERTS + second_grouped, dump_slot).astype(jnp.int32)
    grouped_tokens = tokens.reshape(group_count, TOK_DEV, D)

    def fill(items):
        rows, first_slots, second_slots = items
        buffer = jnp.zeros((dump_slot + 1, D), jnp.bfloat16)
        buffer = buffer.at[first_slots].set(rows).at[second_slots].set(rows)
        return buffer[:dump_slot]

    buffers = lax.map(fill, (grouped_tokens, slot_first, slot_second))
    by_expert = buffers.reshape(group_count, CAP, EXPERTS, D).transpose(2, 0, 1, 3).reshape(EXPERTS, group_count * CAP, D)

    def expert_ffn(items):
        rows, weight_in, weight_out = items
        hidden = jax.nn.relu(jnp.dot(rows, weight_in, preferred_element_type=jnp.float32)).astype(jnp.bfloat16)
        return jnp.dot(hidden, weight_out.T, preferred_element_type=jnp.float32).astype(jnp.bfloat16)

    produced = lax.map(expert_ffn, (by_expert, w_in, w_out))
    returned = produced.reshape(EXPERTS, group_count, CAP, D).transpose(1, 2, 0, 3).reshape(group_count, dump_slot, D)
    returned = jnp.concatenate([returned, jnp.zeros((group_count, 1, D), jnp.bfloat16)], axis=1)

    def combine(items):
        table, first_slots, second_slots, weight_first, weight_second = items
        rows_first = table[first_slots].astype(jnp.float32)
        rows_second = table[second_slots].astype(jnp.float32)
        total = weight_first.astype(jnp.float32)[:, None] * rows_first + weight_second.astype(jnp.float32)[:, None] * rows_second
        return total.astype(jnp.bfloat16)

    mixed = lax.map(combine, (returned, slot_first, slot_second, gate_first.reshape(group_count, TOK_DEV), gate_second.reshape(group_count, TOK_DEV)))
    mixed = mixed.reshape(TOKENS, D)
    mean_prob = jnp.mean(probs, axis=0)
    first_share = jnp.mean((first[:, None] == expert_ids[None, :]).astype(jnp.float32), axis=0)
    aux_loss = EXPERTS * jnp.sum(mean_prob * first_share)
    return mixed, aux_loss
```

```python
import jax
import jax.numpy as jnp
from jax import lax
from jax.sharding import Mesh
from jax.sharding import PartitionSpec as P


EXPERT_DP = ("expert_0", "expert_1", "expert_2", "dp")
PLANE = ("expert_0", "expert_2", "dp")
RING = "expert_1"
SLOTS = 4
ROWS = 96
LAST = ROWS - 1
CHUNKS = ((0, 1, 7, 4), (2, 6, 3, 5))
ORDER = (("out", 0), ("out", 1), ("back", 0), ("back", 1))


def after(value, *earlier):
    return lax.optimization_barrier((value, *earlier))[0]


def shift(value, distance, size):
    if distance % size == 0:
        return value
    return lax.ppermute(value, RING, [(i, (i + distance) % size) for i in range(size)])


def exchange(rows, axes):
    return lax.all_to_all(rows, axes, split_axis=0, concat_axis=0, tiled=True)


def positions(routes, priority, experts):
    group_rows = routes.shape[0]
    expert_grid = lax.broadcasted_iota(jnp.int32, (group_rows, experts), 1)
    first, second = routes[:, 0], routes[:, 1]
    first_hot = (expert_grid == first[:, None]).astype(jnp.float32)
    second_hot = (expert_grid == second[:, None]).astype(jnp.float32)
    ranks = priority[0]
    earlier = (ranks[None, :] < ranks[:, None]).astype(jnp.bfloat16)
    before_first = jnp.dot(
        earlier, first_hot.astype(jnp.bfloat16), preferred_element_type=jnp.float32
    )
    before_second = jnp.dot(
        earlier, second_hot.astype(jnp.bfloat16), preferred_element_type=jnp.float32
    )
    first_load = jnp.sum(first_hot, axis=0)
    load = first_load + jnp.sum(second_hot, axis=0)
    pos_first = jnp.sum(before_first * first_hot, axis=1).astype(jnp.int32)
    pos_second = jnp.sum((before_second + first_load[None, :]) * second_hot, axis=1).astype(
        jnp.int32
    )
    return first, second, first_hot, second_hot, pos_first, pos_second, first_load, load


def expert_ffn(rows, w_in, w_out):
    hidden = jax.nn.relu(jnp.dot(rows, w_in, preferred_element_type=jnp.float32)).astype(
        jnp.bfloat16
    )
    return lax.dot_general(
        hidden, w_out, (((1,), (1,)), ((), ())), preferred_element_type=jnp.float32
    ).astype(jnp.bfloat16)


def dense_mix(tokens, slot_first, slot_second, gate_first, gate_second, w_in, w_out):
    group_rows, width = tokens.shape
    slots = lax.axis_size(EXPERT_DP) * SLOTS
    slot_grid = lax.broadcasted_iota(jnp.int32, (slots, group_rows), 0)
    dispatch = ((slot_grid == slot_first[None, :]) | (slot_grid == slot_second[None, :])).astype(
        jnp.bfloat16
    )
    outgoing = jnp.dot(dispatch, tokens, preferred_element_type=jnp.float32).astype(jnp.bfloat16)
    arrived = exchange(outgoing.reshape(-1, SLOTS, width), EXPERT_DP)
    produced = expert_ffn(arrived.reshape(slots, width), w_in, w_out)
    returned = exchange(produced.reshape(-1, SLOTS, width), EXPERT_DP).reshape(slots, width)
    return combine_rows(returned, slot_first, slot_second, gate_first, gate_second)


def combine_rows(table, row_first, row_second, gate_first, gate_second):
    grid = lax.broadcasted_iota(jnp.int32, (row_first.shape[0], table.shape[0]), 1)
    nothing = jnp.zeros((), jnp.bfloat16)
    combine = jnp.where(grid == row_first[:, None], gate_first[:, None], nothing) + jnp.where(
        grid == row_second[:, None], gate_second[:, None], nothing
    )
    return jnp.dot(combine, table, preferred_element_type=jnp.float32).astype(jnp.bfloat16)


def shards(tokens, routes, priority, router, w_in, w_out):
    group_rows, width = tokens.shape
    experts = router.shape[1]
    w_in, w_out = w_in[0], w_out[0]
    planes = lax.axis_size(RING)
    local = lax.axis_size(PLANE)
    inner = lax.axis_size(("expert_2", "dp"))
    here = lax.axis_index(RING)
    first, second, first_hot, second_hot, pos_first, pos_second, first_load, load = positions(
        routes, priority, experts
    )
    kept = jnp.minimum(load, SLOTS)
    ids = jnp.arange(experts, dtype=jnp.int32)
    plane_of = (ids // inner) % planes
    ahead = (plane_of[:, None] == plane_of[None, :]) & (ids[:, None] < ids[None, :])
    base = jnp.sum(jnp.where(ahead, kept[:, None], 0.0), axis=0)
    crowded = jnp.max(base + kept) > LAST

    def row_of(choice, hot, pos):
        start = jnp.sum(hot * base[None, :], axis=1).astype(jnp.int32)
        distance = ((choice // inner) % planes - here) % planes
        good = (pos < SLOTS) & (start + pos < LAST)
        return jnp.where(good, distance * ROWS + start + pos, -1)

    row_first = row_of(first, first_hot, pos_first)
    row_second = row_of(second, second_hot, pos_second)

    by_plane = kept.reshape(-1, planes, inner).transpose(1, 0, 2).reshape(planes, local)
    order = (here + jnp.arange(planes, dtype=jnp.int32)) % planes
    pick = order[:, None] == jnp.arange(planes, dtype=jnp.int32)[None, :]
    counts = jnp.sum(jnp.where(pick[:, :, None], by_plane[None], 0.0), axis=1)
    counts = jnp.pad(counts, ((0, 0), (0, width - local))).astype(jnp.bfloat16)

    row_grid = lax.broadcasted_iota(jnp.int32, (ROWS, group_rows), 0)

    def packed(distance):
        grid = row_grid + distance * ROWS
        hot = ((grid == row_first[None, :]) | (grid == row_second[None, :])).astype(jnp.bfloat16)
        rows = jnp.dot(hot, tokens, preferred_element_type=jnp.float32).astype(jnp.bfloat16)
        is_last = lax.broadcasted_iota(jnp.int32, (ROWS, width), 0) == LAST
        return jnp.where(is_last, counts[distance][None, :], rows)

    logits = jnp.dot(tokens, router, preferred_element_type=jnp.float32)
    probs = jax.nn.softmax(logits, axis=-1)
    logit_first = jnp.sum(logits * first_hot, axis=1)
    logit_second = jnp.sum(logits * second_hot, axis=1)
    gate_first = jax.nn.sigmoid(logit_first - logit_second).astype(jnp.bfloat16)
    gate_second = jax.nn.sigmoid(logit_second - logit_first).astype(jnp.bfloat16)
    flag = jnp.broadcast_to(crowded.astype(jnp.float32), (experts,))
    statistics = jnp.stack([jnp.sum(probs, axis=0), first_load, flag], axis=0)
    for axis in PLANE:
        statistics = lax.psum(statistics, axis)

    incoming = {}
    for chunk in CHUNKS:
        for d in chunk:
            incoming[d] = shift(packed(d), d, planes)

    hots, produced, back, last = {}, {}, {}, tokens
    for kind, k in ORDER:
        chunk = CHUNKS[k]
        n = len(chunk)
        if kind == "out":
            lower = jnp.arange(local)[:, None] < jnp.arange(local)[None, :]
            sources = []
            for s, d in enumerate(chunk):
                got = incoming[d][LAST, :local].astype(jnp.float32)
                start = jnp.sum(jnp.where(lower, got[:, None], 0.0), axis=0)
                c = jnp.arange(SLOTS, dtype=jnp.float32)[None, :]
                where = start[:, None] + c
                good = (c < got[:, None]) & (where < LAST)
                sources.append(jnp.where(good, where.astype(jnp.int32) + s * ROWS, -1))
            target = jnp.stack(sources, axis=1).reshape(local * n * SLOTS)
            grid = lax.broadcasted_iota(jnp.int32, (local * n * SLOTS, n * ROWS), 1)
            hots[k] = target
            hot = (grid == target[:, None]).astype(jnp.bfloat16)
            table = jnp.concatenate([incoming[d] for d in chunk], axis=0)
            rows = jnp.dot(hot, table, preferred_element_type=jnp.float32).astype(jnp.bfloat16)
            rows = after(rows.reshape(local, n * SLOTS, width), last)
            arrived = exchange(rows, PLANE)
            last = arrived
            rows = expert_ffn(arrived.reshape(local * n * SLOTS, width), w_in, w_out)
            produced[k] = rows.reshape(local, n * SLOTS, width)
        else:
            rows = exchange(after(produced[k], last), PLANE)
            last = rows
            rows = rows.reshape(local * n * SLOTS, width)
            for s, d in enumerate(chunk):
                grid = lax.broadcasted_iota(jnp.int32, (ROWS, local * n * SLOTS), 0) + s * ROWS
                hot = (grid == hots[k][None, :]).astype(jnp.bfloat16)
                home = jnp.dot(hot, rows, preferred_element_type=jnp.float32).astype(jnp.bfloat16)
                back[d] = shift(home, -d, planes)

    sums = jnp.stack([shift(statistics, -d, planes) for d in range(planes)], axis=0)
    sums = jnp.sum(jnp.where(pick[:, :, None, None], sums[:, None], 0.0), axis=0)
    totals = jnp.sum(sums, axis=0)
    all_tokens = group_rows * planes * local
    aux_loss = experts * jnp.sum(totals[0] / all_tokens * (totals[1] / all_tokens))

    def dense(_):
        slot_first = jnp.where(pos_first < SLOTS, first * SLOTS + pos_first, -1)
        slot_second = jnp.where(pos_second < SLOTS, second * SLOTS + pos_second, -1)
        return dense_mix(tokens, slot_first, slot_second, gate_first, gate_second, w_in, w_out)

    def compact(pieces):
        table = jnp.concatenate(pieces, axis=0)
        return combine_rows(table, row_first, row_second, gate_first, gate_second)

    pieces = tuple(back[d] for d in range(planes))
    mixed = lax.cond(totals[2, 0] > 0, dense, compact, pieces)
    return mixed, aux_loss


def solution(mesh):
    torus = Mesh(
        mesh.devices.reshape(4, 8, 2, mesh.shape["dp"]), ("expert_0", "expert_1", "expert_2", "dp")
    )
    placed = (
        P(EXPERT_DP, None),
        P(EXPERT_DP, None),
        P(EXPERT_DP, None),
        P(),
        P(EXPERT_DP, None, None),
        P(EXPERT_DP, None, None),
    )
    return jax.shard_map(
        shards, mesh=torus, in_specs=placed, out_specs=(P(EXPERT_DP, None), P()), check_vma=False
    )
```

```python
import functools

import jax
import jax.numpy as jnp
from jax import lax
from jax.experimental import pallas as pl
from jax.experimental.pallas import tpu as pltpu
from jax.sharding import Mesh
from jax.sharding import PartitionSpec as P


EXPERT_DP = ("expert_0", "expert_1", "expert_2", "dp")
ROUTE = ("expert_2", "expert_0", "dp", "expert_1")
PLANE = ("expert_0", "expert_2", "dp")
RING = "expert_1"
SLOTS = 4
HALVES = 2
BLOCK = SLOTS * HALVES
STEP = 256


def number(expert, sizes):
    planes, cores, columns = sizes["expert_1"], sizes["expert_2"], sizes["dp"]
    y = expert % columns
    core = (expert // columns) % cores
    z = (expert // (columns * cores)) % planes
    x = expert // (columns * cores * planes)
    return ((core * sizes["expert_0"] + x) * columns + y) * planes + z


def dispatch_kernel(routes_ref, ranks_ref, tokens_ref, out_ref, codes_ref, *, sizes):
    group, width = tokens_ref.shape
    half = width // HALVES
    experts = out_ref.shape[0] * pl.num_programs(0) // BLOCK

    @pl.when(pl.program_id(0) == 0)
    def _():
        first = routes_ref[0:1, :]
        second = routes_ref[1:2, :]
        ids = lax.broadcasted_iota(jnp.int32, (experts, group), 0)
        first_hot = jnp.where(ids == first, 1.0, 0.0)
        second_hot = jnp.where(ids == second, 1.0, 0.0)
        rows = lax.broadcasted_iota(jnp.int32, (group, group), 0)
        lanes = lax.broadcasted_iota(jnp.int32, (group, group), 1)
        ranks = ranks_ref[...].astype(jnp.float32)
        column = jnp.sum(jnp.where(rows == lanes, ranks, 0.0), axis=1, keepdims=True)
        earlier = jnp.where(column < ranks, 1.0, 0.0).astype(jnp.bfloat16)
        before_first = jnp.dot(
            first_hot.astype(jnp.bfloat16), earlier, preferred_element_type=jnp.float32
        )
        before_second = jnp.dot(
            second_hot.astype(jnp.bfloat16), earlier, preferred_element_type=jnp.float32
        )
        load = jnp.sum(first_hot, axis=1, keepdims=True)
        pos_first = jnp.sum(before_first * first_hot, axis=0, keepdims=True).astype(jnp.int32)
        pos_second = jnp.sum((before_second + load) * second_hot, axis=0, keepdims=True).astype(
            jnp.int32
        )
        codes_ref[0:1, :] = jnp.where(
            pos_first < SLOTS, number(first, sizes) * BLOCK + pos_first, -BLOCK
        )
        codes_ref[1:2, :] = jnp.where(
            pos_second < SLOTS, number(second, sizes) * BLOCK + pos_second, -BLOCK
        )

    count = out_ref.shape[0]
    here = lax.broadcasted_iota(jnp.int32, (count, group), 0) + pl.program_id(0) * count
    first, second = codes_ref[0:1, :], codes_ref[1:2, :]
    total = jnp.zeros((count, half), jnp.float32)
    for h in range(HALVES):
        hit = (here == first + h * SLOTS) | (here == second + h * SLOTS)
        hot = jnp.where(hit, 1.0, 0.0).astype(jnp.bfloat16)
        total += jnp.dot(
            hot, tokens_ref[:, h * half : (h + 1) * half], preferred_element_type=jnp.float32
        )
    out_ref[...] = total.astype(jnp.bfloat16)


def dispatch(routes, ranks, tokens, experts, sizes):
    group, width = tokens.shape
    rows = experts * BLOCK
    return pl.pallas_call(
        functools.partial(dispatch_kernel, sizes=sizes),
        grid=(rows // STEP,),
        in_specs=[
            pl.BlockSpec((2, group), lambda i: (0, 0)),
            pl.BlockSpec((1, group), lambda i: (0, 0)),
            pl.BlockSpec((group, width), lambda i: (0, 0)),
        ],
        out_specs=[
            pl.BlockSpec((STEP, width // HALVES), lambda i: (i, 0)),
            pl.BlockSpec((2, group), lambda i: (0, 0)),
        ],
        out_shape=[
            jax.ShapeDtypeStruct((rows, width // HALVES), jnp.bfloat16),
            jax.ShapeDtypeStruct((2, group), jnp.int32),
        ],
        compiler_params=pltpu.CompilerParams(dimension_semantics=("arbitrary",)),
        name="dispatch",
    )(routes, ranks, tokens)


def ffn_kernel(x_ref, w_in_ref, w_out_ref, out_ref, low_ref, high_ref):
    half = x_ref.shape[1]
    part = STEP // HALVES
    to_row = lax.broadcasted_iota(jnp.int32, (STEP, STEP), 0)
    from_row = lax.broadcasted_iota(jnp.int32, (STEP, STEP), 1)
    slot, source, side = to_row % SLOTS, (to_row % part) // SLOTS, to_row // part
    sort = jnp.where(from_row == source * BLOCK + side * SLOTS + slot, 1.0, 0.0)
    slot, side, source = from_row % SLOTS, from_row // part, (from_row % part) // SLOTS
    unsort = jnp.where(to_row == source * BLOCK + side * SLOTS + slot, 1.0, 0.0)
    sort, unsort = sort.astype(jnp.bfloat16), unsort.astype(jnp.bfloat16)
    subs = x_ref.shape[0] // STEP
    for s in range(subs):
        rows = jnp.dot(
            sort, x_ref[s * STEP : (s + 1) * STEP, :], preferred_element_type=jnp.float32
        ).astype(jnp.bfloat16)
        low_ref[s * part : (s + 1) * part, :] = rows[:part]
        high_ref[s * part : (s + 1) * part, :] = rows[part:]
    hidden = jnp.dot(low_ref[...], w_in_ref[:half, :], preferred_element_type=jnp.float32)
    hidden += jnp.dot(high_ref[...], w_in_ref[half:, :], preferred_element_type=jnp.float32)
    hidden = jnp.maximum(hidden, 0.0).astype(jnp.bfloat16)
    transposed = (((1,), (1,)), ((), ()))
    low_ref[...] = lax.dot_general(
        hidden, w_out_ref[:half, :], transposed, preferred_element_type=jnp.float32
    ).astype(jnp.bfloat16)
    high_ref[...] = lax.dot_general(
        hidden, w_out_ref[half:, :], transposed, preferred_element_type=jnp.float32
    ).astype(jnp.bfloat16)
    for s in range(subs):
        span = slice(s * part, (s + 1) * part)
        rows = jnp.concatenate([low_ref[span, :], high_ref[span, :]], axis=0)
        out_ref[s * STEP : (s + 1) * STEP, :] = jnp.dot(
            unsort, rows, preferred_element_type=jnp.float32
        ).astype(jnp.bfloat16)


def expert_ffn(rows, w_in, w_out, steps=4):
    count, half = rows.shape
    chunk = count // steps
    return pl.pallas_call(
        ffn_kernel,
        grid=(steps,),
        in_specs=[
            pl.BlockSpec((chunk, half), lambda i: (i, 0)),
            pl.BlockSpec(w_in.shape, lambda i: (0, 0)),
            pl.BlockSpec(w_out.shape, lambda i: (0, 0)),
        ],
        out_specs=pl.BlockSpec((chunk, half), lambda i: (i, 0)),
        out_shape=jax.ShapeDtypeStruct((count, half), jnp.bfloat16),
        scratch_shapes=[
            pltpu.VMEM((chunk // HALVES, half), jnp.bfloat16),
            pltpu.VMEM((chunk // HALVES, half), jnp.bfloat16),
        ],
        compiler_params=pltpu.CompilerParams(
            dimension_semantics=("arbitrary",), vmem_limit_bytes=48 << 20
        ),
        name="ffn",
    )(rows, w_in, w_out)


def combine_kernel(codes_ref, gates_ref, table_ref, out_ref, weights_ref):
    group = codes_ref.shape[0]
    count, span = table_ref.shape
    half = out_ref.shape[1] // HALVES

    @pl.when(pl.program_id(0) == 0)
    def _():
        here = lax.broadcasted_iota(jnp.int32, (group, count), 1)
        for h in range(HALVES):
            total = jnp.where(here == codes_ref[:, 0:1] + h * SLOTS, gates_ref[:, 0:1], 0.0)
            total += jnp.where(here == codes_ref[:, 1:2] + h * SLOTS, gates_ref[:, 1:2], 0.0)
            weights_ref[h] = total.astype(jnp.bfloat16)

    for h in range(HALVES):
        start = pl.multiple_of(h * half + pl.program_id(0) * span, 128)
        out_ref[:, pl.ds(start, span)] = jnp.dot(
            weights_ref[h], table_ref[...], preferred_element_type=jnp.float32
        ).astype(jnp.bfloat16)


def combine(codes, gates, table, steps=4):
    group = codes.shape[0]
    count, half = table.shape
    return pl.pallas_call(
        combine_kernel,
        grid=(steps,),
        in_specs=[
            pl.BlockSpec((group, 2), lambda i: (0, 0)),
            pl.BlockSpec((group, 2), lambda i: (0, 0)),
            pl.BlockSpec((count, half // steps), lambda i: (0, i)),
        ],
        out_specs=pl.BlockSpec((group, half * HALVES), lambda i: (0, 0)),
        out_shape=jax.ShapeDtypeStruct((group, half * HALVES), jnp.bfloat16),
        scratch_shapes=[pltpu.VMEM((HALVES, group, count), jnp.bfloat16)],
        compiler_params=pltpu.CompilerParams(dimension_semantics=("arbitrary",)),
        name="combine",
    )(codes, gates, table)


def exchange(rows):
    count, half = rows.shape
    blocks = rows.reshape(count // BLOCK, BLOCK, half)
    blocks = lax.all_to_all(blocks, ROUTE, split_axis=0, concat_axis=0, tiled=True)
    return blocks.reshape(count, half)


def shards(tokens, routes, priority, router, w_in, w_out):
    group = tokens.shape[0]
    experts = router.shape[1]
    sizes = {axis: lax.axis_size(axis) for axis in EXPERT_DP}
    planes = sizes[RING]
    outgoing, codes = dispatch(routes.T, priority, tokens, experts, sizes)
    arrived = exchange(outgoing)

    late, codes, routes, _ = lax.optimization_barrier((tokens, codes, routes, outgoing))
    logits = jnp.dot(late, router, preferred_element_type=jnp.float32)
    probs = jax.nn.softmax(logits, axis=-1)
    expert_grid = lax.broadcasted_iota(jnp.int32, (group, experts), 1)
    first_hot = (expert_grid == routes[:, 0:1]).astype(jnp.float32)
    second_hot = (expert_grid == routes[:, 1:2]).astype(jnp.float32)
    logit_first = jnp.sum(logits * first_hot, axis=1)
    logit_second = jnp.sum(logits * second_hot, axis=1)
    gates = jnp.stack(
        [
            jax.nn.sigmoid(logit_first - logit_second),
            jax.nn.sigmoid(logit_second - logit_first),
        ],
        axis=1,
    )
    gates = gates.astype(jnp.bfloat16).astype(jnp.float32)
    statistics = jnp.stack([jnp.sum(probs, axis=0), jnp.sum(first_hot, axis=0)], axis=0)
    for axis in PLANE:
        statistics = lax.psum(statistics, axis)
    arrived, statistics, codes, gates = lax.optimization_barrier(
        (arrived, statistics, codes.T, gates)
    )
    produced = expert_ffn(arrived, w_in[0], w_out[0])
    sums = [statistics]
    for d in range(1, planes):
        ring = [(i, (i - d) % planes) for i in range(planes)]
        sums.append(lax.ppermute(statistics, RING, ring))
    returned = exchange(produced)
    mixed = combine(codes, gates, returned)

    order = (lax.axis_index(RING) + jnp.arange(planes, dtype=jnp.int32)) % planes
    pick = order[:, None] == jnp.arange(planes, dtype=jnp.int32)[None, :]
    sums = jnp.stack(sums, axis=0)
    totals = jnp.sum(
        jnp.sum(jnp.where(pick[:, :, None, None], sums[:, None], 0.0), axis=0), axis=0
    )
    all_tokens = group * experts
    aux_loss = experts * jnp.sum(totals[0] / all_tokens * (totals[1] / all_tokens))
    return mixed, aux_loss


def solution(mesh):
    torus = Mesh(
        mesh.devices.reshape(4, 8, 2, mesh.shape["dp"]), ("expert_0", "expert_1", "expert_2", "dp")
    )
    placed = (
        P(EXPERT_DP, None),
        P(EXPERT_DP, None),
        P(EXPERT_DP, None),
        P(),
        P(EXPERT_DP, None, None),
        P(EXPERT_DP, None, None),
    )
    return jax.shard_map(
        shards, mesh=torus, in_specs=placed, out_specs=(P(EXPERT_DP, None), P()), check_vma=False
    )
```

```python
import functools

import jax
import jax.numpy as jnp
from jax import lax
from jax.experimental import pallas as pl
from jax.experimental.pallas import tpu as pltpu
from jax.sharding import Mesh
from jax.sharding import PartitionSpec as P


EXPERT_DP = ("expert_0", "expert_1", "expert_2", "dp")
ROUTE = ("expert_2", "expert_0", "dp", "expert_1")
PLANE = ("expert_0", "expert_2", "dp")
RING = "expert_1"
SLOTS = 4
HALVES = 2
BLOCK = SLOTS * HALVES
STEPS = 4
DSTEPS = 8
SPAN = 512


def number(expert, sizes):
    planes, cores, columns = sizes["expert_1"], sizes["expert_2"], sizes["dp"]
    y = expert % columns
    core = (expert // columns) % cores
    z = (expert // (columns * cores)) % planes
    x = expert // (columns * cores * planes)
    return ((core * sizes["expert_0"] + x) * columns + y) * planes + z


def dispatch_kernel(routes_ref, ranks_ref, tokens_hbm, out_hbm, codes_ref, tokens_ref, out_ref, t_sem, o_sem, *, sizes):
    group, width = tokens_ref.shape
    half = width // HALVES
    steps = o_sem.shape[0]
    chunk = out_ref.shape[0] // steps
    experts = out_ref.shape[0] // BLOCK
    count = chunk // HALVES
    load = pltpu.make_async_copy(tokens_hbm, tokens_ref, t_sem)
    load.start()
    first = routes_ref[0:1, :]
    second = routes_ref[1:2, :]
    ids = lax.broadcasted_iota(jnp.int32, (experts, group), 0)
    first_hot = jnp.where(ids == first, 1.0, 0.0)
    second_hot = jnp.where(ids == second, 1.0, 0.0)
    rows = lax.broadcasted_iota(jnp.int32, (group, group), 0)
    lanes = lax.broadcasted_iota(jnp.int32, (group, group), 1)
    ranks = ranks_ref[...].astype(jnp.float32)
    column = jnp.sum(jnp.where(rows == lanes, ranks, 0.0), axis=1, keepdims=True)
    earlier = jnp.where(column < ranks, 1.0, 0.0).astype(jnp.bfloat16)
    before_first = jnp.dot(
        first_hot.astype(jnp.bfloat16), earlier, preferred_element_type=jnp.float32
    )
    before_second = jnp.dot(
        second_hot.astype(jnp.bfloat16), earlier, preferred_element_type=jnp.float32
    )
    first_load = jnp.sum(first_hot, axis=1, keepdims=True)
    pos_first = jnp.sum(before_first * first_hot, axis=0, keepdims=True).astype(jnp.int32)
    pos_second = jnp.sum((before_second + first_load) * second_hot, axis=0, keepdims=True).astype(
        jnp.int32
    )
    slot_first = jnp.where(pos_first < SLOTS, number(first, sizes) * SLOTS + pos_first, -1)
    slot_second = jnp.where(pos_second < SLOTS, number(second, sizes) * SLOTS + pos_second, -1)
    codes_ref[0:1, :] = slot_first
    codes_ref[1:2, :] = slot_second
    load.wait()
    copies = []
    for i in range(steps):
        here = lax.broadcasted_iota(jnp.int32, (count, group), 0) + i * count
        hot = jnp.where((here == slot_first) | (here == slot_second), 1.0, 0.0)
        hot = hot.astype(jnp.bfloat16)
        span = SPAN
        for j in range(half // span):
            sides = []
            for h in range(HALVES):
                cols = slice(h * half + j * span, h * half + (j + 1) * span)
                side = jnp.dot(hot, tokens_ref[:, cols], preferred_element_type=jnp.float32)
                sides.append(side.reshape(count // SLOTS, 1, SLOTS, span))
            out_ref[i * chunk : (i + 1) * chunk, j * span : (j + 1) * span] = (
                jnp.concatenate(sides, axis=1).reshape(chunk, span).astype(jnp.bfloat16)
            )
        part = pl.ds(i * chunk, chunk)
        copies.append(
            pltpu.make_async_copy(out_ref.at[part, :], out_hbm.at[part, :], o_sem.at[i])
        )
        copies[-1].start()
    for copy in copies:
        copy.wait()


def dispatch(routes, ranks, tokens, experts, sizes):
    group, width = tokens.shape
    rows, half = experts * BLOCK, width // HALVES
    hbm = pl.BlockSpec(memory_space=pltpu.HBM)
    vmem = pl.BlockSpec(memory_space=pltpu.VMEM)
    return pl.pallas_call(
        functools.partial(dispatch_kernel, sizes=sizes),
        in_specs=[vmem, vmem, hbm],
        out_specs=[hbm, vmem],
        out_shape=[
            pltpu.HBM((rows, half), jnp.bfloat16),
            jax.ShapeDtypeStruct((2, group), jnp.int32),
        ],
        scratch_shapes=[
            pltpu.VMEM((group, width), jnp.bfloat16),
            pltpu.VMEM((rows, half), jnp.bfloat16),
            pltpu.SemaphoreType.DMA,
            pltpu.SemaphoreType.DMA((DSTEPS,)),
        ],
        name="dispatch",
    )(routes, ranks, tokens)


def ffn_kernel(
    x_hbm,
    w_in_hbm,
    w_out_hbm,
    out_hbm,
    x_ref,
    w_in_ref,
    w_out_ref,
    y_ref,
    sorted_ref,
    hidden_ref,
    x_sem,
    in_sem,
    foot_sem,
    y_sem,
):
    half = x_ref.shape[1]
    steps = x_sem.shape[0]
    chunk = x_ref.shape[0] // steps
    blocks = chunk // BLOCK
    count = blocks * SLOTS
    transposed = (((1,), (1,)), ((), ()))

    def x_copy(i):
        rows = pl.ds(i * chunk, chunk)
        return pltpu.make_async_copy(x_hbm.at[rows, :], x_ref.at[rows, :], x_sem.at[i])

    def y_copy(i):
        rows = pl.ds(i * chunk, chunk)
        return pltpu.make_async_copy(y_ref.at[rows, :], out_hbm.at[rows, :], y_sem.at[i])

    def in_copy(j):
        cols = pl.ds(j * SPAN, SPAN)
        return pltpu.make_async_copy(w_in_hbm.at[:, cols], w_in_ref.at[:, cols], in_sem.at[j])

    def foot_copy(h):
        rows = pl.ds(h * half, half)
        return pltpu.make_async_copy(w_out_hbm.at[rows, :], w_out_ref.at[rows, :], foot_sem.at[h])

    x_copy(0).start()
    for j in range(in_sem.shape[0]):
        in_copy(j).start()
    for i in range(steps):
        top = i * chunk
        x_copy(i).wait()
        if i == 0:
            for h in range(HALVES):
                foot_copy(h).start()
        rows = x_ref[top : top + chunk, :].astype(jnp.float32)
        rows = rows.reshape(blocks, HALVES, SLOTS, half)
        for h in range(HALVES):
            sorted_ref[:, h * half : (h + 1) * half] = (
                rows[:, h].reshape(count, half).astype(jnp.bfloat16)
            )
        for j in range(w_in_ref.shape[1] // SPAN):
            if i == 0:
                in_copy(j).wait()
            cols = slice(j * SPAN, (j + 1) * SPAN)
            total = jnp.dot(sorted_ref[...], w_in_ref[:, cols], preferred_element_type=jnp.float32)
            hidden_ref[:, cols] = jnp.maximum(total, 0.0).astype(jnp.bfloat16)
        if i + 1 < steps:
            x_copy(i + 1).start()
        for j in range(half // SPAN):
            sides = []
            for h in range(HALVES):
                if i == 0 and j == 0:
                    foot_copy(h).wait()
                feet = slice(h * half + j * SPAN, h * half + (j + 1) * SPAN)
                side = lax.dot_general(
                    hidden_ref[...],
                    w_out_ref[feet, :],
                    transposed,
                    preferred_element_type=jnp.float32,
                )
                sides.append(side.reshape(blocks, 1, SLOTS, SPAN))
            y_ref[top : top + chunk, j * SPAN : (j + 1) * SPAN] = (
                jnp.concatenate(sides, axis=1).reshape(chunk, SPAN).astype(jnp.bfloat16)
            )
        y_copy(i).start()
    for i in range(steps):
        y_copy(i).wait()


def expert_ffn(rows, w_in, w_out):
    count, half = rows.shape
    chunk = count // STEPS
    hbm = pl.BlockSpec(memory_space=pltpu.HBM)
    return pl.pallas_call(
        ffn_kernel,
        in_specs=[hbm, hbm, hbm],
        out_specs=hbm,
        out_shape=pltpu.HBM((count, half), jnp.bfloat16),
        scratch_shapes=[
            pltpu.VMEM((count, half), jnp.bfloat16),
            pltpu.VMEM(w_in.shape, jnp.bfloat16),
            pltpu.VMEM(w_out.shape, jnp.bfloat16),
            pltpu.VMEM((count, half), jnp.bfloat16),
            pltpu.VMEM((chunk // HALVES, half * HALVES), jnp.bfloat16),
            pltpu.VMEM((chunk // HALVES, w_in.shape[1]), jnp.bfloat16),
            pltpu.SemaphoreType.DMA((STEPS,)),
            pltpu.SemaphoreType.DMA((w_in.shape[1] // SPAN,)),
            pltpu.SemaphoreType.DMA((HALVES,)),
            pltpu.SemaphoreType.DMA((STEPS,)),
        ],
        name="ffn",
    )(rows, w_in, w_out)


def mixing_kernel(codes_ref, gates_ref, out_ref):
    halves, group, count = out_ref.shape
    here = lax.broadcasted_iota(jnp.int32, (group, count), 1)
    slot = here // BLOCK * SLOTS + here % SLOTS
    side = here // SLOTS % HALVES
    total = jnp.where(slot == codes_ref[:, 0:1], gates_ref[:, 0:1], 0.0)
    total = jnp.where(slot == codes_ref[:, 1:2], gates_ref[:, 1:2], total)
    for h in range(halves):
        out_ref[h] = jnp.where(side == h, total, 0.0).astype(jnp.bfloat16)


def mixing(codes, gates, count):
    vmem = pl.BlockSpec(memory_space=pltpu.VMEM)
    return pl.pallas_call(
        mixing_kernel,
        in_specs=[vmem, vmem],
        out_specs=vmem,
        out_shape=pltpu.HBM((HALVES, codes.shape[0], count), jnp.bfloat16),
        name="mixing",
    )(codes, gates)


def combine_kernel(
    weights_hbm, table_hbm, out_hbm, weights_ref, table_ref, out_ref, w_sem, in_sem, out_sem
):
    half = table_ref.shape[1]
    parts = in_sem.shape[0]
    span = half // parts

    def load(j):
        cols = pl.ds(j * span, span)
        return pltpu.make_async_copy(table_hbm.at[:, cols], table_ref.at[:, cols], in_sem.at[j])

    def store(h, j):
        cols = pl.ds(h * half + j * span, span)
        return pltpu.make_async_copy(out_ref.at[:, cols], out_hbm.at[:, cols], out_sem.at[h, j])

    def weigh(h):
        return pltpu.make_async_copy(weights_hbm.at[h], weights_ref.at[h], w_sem.at[h])

    load(0).start()
    for h in range(HALVES):
        weigh(h).start()
    for j in range(1, parts):
        load(j).start()
    for j in range(parts):
        load(j).wait()
        for h in range(HALVES):
            if j == 0:
                weigh(h).wait()
            start = h * half + j * span
            out_ref[:, start : start + span] = jnp.dot(
                weights_ref[h],
                table_ref[:, j * span : (j + 1) * span],
                preferred_element_type=jnp.float32,
            ).astype(jnp.bfloat16)
            store(h, j).start()
    for j in range(parts):
        for h in range(HALVES):
            store(h, j).wait()


def combine(weights, table):
    group = weights.shape[1]
    count, half = table.shape
    hbm = pl.BlockSpec(memory_space=pltpu.HBM)
    return pl.pallas_call(
        combine_kernel,
        in_specs=[hbm, hbm],
        out_specs=hbm,
        out_shape=pltpu.HBM((group, half * HALVES), jnp.bfloat16),
        scratch_shapes=[
            pltpu.VMEM(weights.shape, jnp.bfloat16),
            pltpu.VMEM((count, half), jnp.bfloat16),
            pltpu.VMEM((group, half * HALVES), jnp.bfloat16),
            pltpu.SemaphoreType.DMA((HALVES,)),
            pltpu.SemaphoreType.DMA((half // SPAN,)),
            pltpu.SemaphoreType.DMA((HALVES, half // SPAN)),
        ],
        name="combine",
    )(weights, table)


def exchange(rows):
    count, half = rows.shape
    blocks = rows.reshape(count // BLOCK, BLOCK, half)
    blocks = lax.all_to_all(blocks, ROUTE, split_axis=0, concat_axis=0, tiled=True)
    return blocks.reshape(count, half)


def shards(tokens, routes, priority, router, w_in, w_out):
    group = tokens.shape[0]
    experts = router.shape[1]
    sizes = {axis: lax.axis_size(axis) for axis in EXPERT_DP}
    planes = sizes[RING]
    outgoing, codes = dispatch(routes.T, priority, tokens, experts, sizes)
    arrived = exchange(outgoing)

    late, codes, routes, _ = lax.optimization_barrier((tokens, codes, routes, outgoing))
    logits = jnp.dot(late, router, preferred_element_type=jnp.float32)
    probs = jax.nn.softmax(logits, axis=-1)
    expert_grid = lax.broadcasted_iota(jnp.int32, (group, experts), 1)
    first_hot = (expert_grid == routes[:, 0:1]).astype(jnp.float32)
    second_hot = (expert_grid == routes[:, 1:2]).astype(jnp.float32)
    logit_first = jnp.sum(logits * first_hot, axis=1)
    logit_second = jnp.sum(logits * second_hot, axis=1)
    gates = jnp.stack(
        [
            jax.nn.sigmoid(logit_first - logit_second),
            jax.nn.sigmoid(logit_second - logit_first),
        ],
        axis=1,
    )
    gates = gates.astype(jnp.bfloat16).astype(jnp.float32)
    statistics = jnp.stack([jnp.sum(probs, axis=0), jnp.sum(first_hot, axis=0)], axis=0)
    for axis in PLANE:
        statistics = lax.psum(statistics, axis)
    mixers = mixing(codes.T, gates, outgoing.shape[0])
    arrived, statistics, mixers = lax.optimization_barrier((arrived, statistics, mixers))
    produced = expert_ffn(arrived, w_in[0], w_out[0])
    sums = [statistics]
    for d in range(1, planes):
        ring = [(i, (i - d) % planes) for i in range(planes)]
        sums.append(lax.ppermute(statistics, RING, ring))
    returned = exchange(produced)
    mixed = combine(mixers, returned)

    order = (lax.axis_index(RING) + jnp.arange(planes, dtype=jnp.int32)) % planes
    pick = order[:, None] == jnp.arange(planes, dtype=jnp.int32)[None, :]
    sums = jnp.stack(sums, axis=0)
    totals = jnp.sum(
        jnp.sum(jnp.where(pick[:, :, None, None], sums[:, None], 0.0), axis=0), axis=0
    )
    all_tokens = group * experts
    aux_loss = experts * jnp.sum(totals[0] / all_tokens * (totals[1] / all_tokens))
    return mixed, aux_loss


def solution(mesh):
    torus = Mesh(
        mesh.devices.reshape(4, 8, 2, mesh.shape["dp"]), ("expert_0", "expert_1", "expert_2", "dp")
    )
    placed = (
        P(EXPERT_DP, None),
        P(EXPERT_DP, None),
        P(EXPERT_DP, None),
        P(),
        P(EXPERT_DP, None, None),
        P(EXPERT_DP, None, None),
    )
    return jax.shard_map(
        shards, mesh=torus, in_specs=placed, out_specs=(P(EXPERT_DP, None), P()), check_vma=False
    )
```

```python
import functools

import jax
import jax.numpy as jnp
from jax import lax
from jax.experimental import pallas as pl
from jax.experimental.pallas import tpu as pltpu
from jax.sharding import Mesh
from jax.sharding import PartitionSpec as P


EXPERT_DP = ("expert_0", "expert_1", "expert_2", "dp")
ROUTE = ("expert_2", "expert_0", "dp", "expert_1")
PLANE = ("expert_0", "expert_2", "dp")
RING = "expert_1"
SLOTS = 4
HALVES = 2
BLOCK = SLOTS * HALVES
STEPS = 4
DSTEPS = 8
SPAN = 512


def number(expert, sizes):
    planes, cores, columns = sizes["expert_1"], sizes["expert_2"], sizes["dp"]
    y = expert % columns
    core = (expert // columns) % cores
    z = (expert // (columns * cores)) % planes
    x = expert // (columns * cores * planes)
    return ((core * sizes["expert_0"] + x) * columns + y) * planes + z


def dispatch_kernel(routes_ref, ranks_ref, tokens_hbm, out_hbm, codes_ref, tokens_ref, out_ref, t_sem, o_sem, *, sizes):
    group, width = tokens_ref.shape
    half = width // HALVES
    steps = o_sem.shape[0]
    chunk = out_ref.shape[0] // steps
    experts = out_ref.shape[0] // BLOCK
    count = chunk // HALVES
    load = pltpu.make_async_copy(tokens_hbm, tokens_ref, t_sem)
    load.start()
    first = routes_ref[0:1, :]
    second = routes_ref[1:2, :]
    ids = lax.broadcasted_iota(jnp.int32, (experts, group), 0)
    first_hot = jnp.where(ids == first, 1.0, 0.0)
    second_hot = jnp.where(ids == second, 1.0, 0.0)
    rows = lax.broadcasted_iota(jnp.int32, (group, group), 0)
    lanes = lax.broadcasted_iota(jnp.int32, (group, group), 1)
    ranks = ranks_ref[...].astype(jnp.float32)
    column = jnp.sum(jnp.where(rows == lanes, ranks, 0.0), axis=1, keepdims=True)
    earlier = jnp.where(column < ranks, 1.0, 0.0).astype(jnp.bfloat16)
    before_first = jnp.dot(
        first_hot.astype(jnp.bfloat16), earlier, preferred_element_type=jnp.float32
    )
    before_second = jnp.dot(
        second_hot.astype(jnp.bfloat16), earlier, preferred_element_type=jnp.float32
    )
    first_load = jnp.sum(first_hot, axis=1, keepdims=True)
    pos_first = jnp.sum(before_first * first_hot, axis=0, keepdims=True).astype(jnp.int32)
    pos_second = jnp.sum((before_second + first_load) * second_hot, axis=0, keepdims=True).astype(
        jnp.int32
    )
    slot_first = jnp.where(pos_first < SLOTS, number(first, sizes) * SLOTS + pos_first, -1)
    slot_second = jnp.where(pos_second < SLOTS, number(second, sizes) * SLOTS + pos_second, -1)
    codes_ref[0:1, :] = slot_first
    codes_ref[1:2, :] = slot_second
    load.wait()
    copies = []
    for i in range(steps):
        here = lax.broadcasted_iota(jnp.int32, (count, group), 0) + i * count
        hot = jnp.where((here == slot_first) | (here == slot_second), 1.0, 0.0)
        hot = hot.astype(jnp.bfloat16)
        span = SPAN
        for j in range(half // span):
            sides = []
            for h in range(HALVES):
                cols = slice(h * half + j * span, h * half + (j + 1) * span)
                side = jnp.dot(hot, tokens_ref[:, cols], preferred_element_type=jnp.float32)
                sides.append(side.reshape(count // SLOTS, 1, SLOTS, span))
            out_ref[i * chunk : (i + 1) * chunk, j * span : (j + 1) * span] = (
                jnp.concatenate(sides, axis=1).reshape(chunk, span).astype(jnp.bfloat16)
            )
        part = pl.ds(i * chunk, chunk)
        copies.append(
            pltpu.make_async_copy(out_ref.at[part, :], out_hbm.at[part, :], o_sem.at[i])
        )
        copies[-1].start()
    for copy in copies:
        copy.wait()


def dispatch(routes, ranks, tokens, experts, sizes):
    group, width = tokens.shape
    rows, half = experts * BLOCK, width // HALVES
    hbm = pl.BlockSpec(memory_space=pltpu.HBM)
    vmem = pl.BlockSpec(memory_space=pltpu.VMEM)
    return pl.pallas_call(
        functools.partial(dispatch_kernel, sizes=sizes),
        in_specs=[vmem, vmem, hbm],
        out_specs=[hbm, vmem],
        out_shape=[
            pltpu.HBM((rows, half), jnp.bfloat16),
            jax.ShapeDtypeStruct((2, group), jnp.int32),
        ],
        scratch_shapes=[
            pltpu.VMEM((group, width), jnp.bfloat16),
            pltpu.VMEM((rows, half), jnp.bfloat16),
            pltpu.SemaphoreType.DMA,
            pltpu.SemaphoreType.DMA((DSTEPS,)),
        ],
        name="dispatch",
    )(routes, ranks, tokens)


def ffn_kernel(
    x_hbm,
    w_in_hbm,
    w_out_hbm,
    y_ref,
    x_ref,
    w_in_ref,
    w_out_ref,
    sorted_ref,
    hidden_ref,
    x_sem,
    in_sem,
    foot_sem,
):
    half = x_ref.shape[1]
    steps = x_sem.shape[0]
    chunk = x_ref.shape[0] // steps
    blocks = chunk // BLOCK
    count = blocks * SLOTS
    transposed = (((1,), (1,)), ((), ()))

    def x_copy(i):
        rows = pl.ds(i * chunk, chunk)
        return pltpu.make_async_copy(x_hbm.at[rows, :], x_ref.at[rows, :], x_sem.at[i])

    def in_copy(j):
        cols = pl.ds(j * SPAN, SPAN)
        return pltpu.make_async_copy(w_in_hbm.at[:, cols], w_in_ref.at[:, cols], in_sem.at[j])

    def foot_copy(h):
        rows = pl.ds(h * half, half)
        return pltpu.make_async_copy(w_out_hbm.at[rows, :], w_out_ref.at[rows, :], foot_sem.at[h])

    x_copy(0).start()
    for j in range(in_sem.shape[0]):
        in_copy(j).start()
    for i in range(steps):
        top = i * chunk
        x_copy(i).wait()
        if i == 0:
            for h in range(HALVES):
                foot_copy(h).start()
        rows = x_ref[top : top + chunk, :].astype(jnp.float32)
        rows = rows.reshape(blocks, HALVES, SLOTS, half)
        for h in range(HALVES):
            sorted_ref[:, h * half : (h + 1) * half] = (
                rows[:, h].reshape(count, half).astype(jnp.bfloat16)
            )
        for j in range(w_in_ref.shape[1] // SPAN):
            if i == 0:
                in_copy(j).wait()
            cols = slice(j * SPAN, (j + 1) * SPAN)
            total = jnp.dot(sorted_ref[...], w_in_ref[:, cols], preferred_element_type=jnp.float32)
            hidden_ref[:, cols] = jnp.maximum(total, 0.0).astype(jnp.bfloat16)
        if i + 1 < steps:
            x_copy(i + 1).start()
        for j in range(half // SPAN):
            sides = []
            for h in range(HALVES):
                if i == 0 and j == 0:
                    foot_copy(h).wait()
                feet = slice(h * half + j * SPAN, h * half + (j + 1) * SPAN)
                side = lax.dot_general(
                    hidden_ref[...],
                    w_out_ref[feet, :],
                    transposed,
                    preferred_element_type=jnp.float32,
                )
                sides.append(side.reshape(blocks, 1, SLOTS, SPAN))
            y_ref[top : top + chunk, j * SPAN : (j + 1) * SPAN] = (
                jnp.concatenate(sides, axis=1).reshape(chunk, SPAN).astype(jnp.bfloat16)
            )


def expert_ffn(rows, w_in, w_out):
    count, half = rows.shape
    chunk = count // STEPS
    hbm = pl.BlockSpec(memory_space=pltpu.HBM)
    return pl.pallas_call(
        ffn_kernel,
        in_specs=[hbm, hbm, hbm],
        out_specs=pl.BlockSpec(memory_space=pltpu.VMEM),
        out_shape=pltpu.VMEM((count, half), jnp.bfloat16),
        scratch_shapes=[
            pltpu.VMEM((count, half), jnp.bfloat16),
            pltpu.VMEM(w_in.shape, jnp.bfloat16),
            pltpu.VMEM(w_out.shape, jnp.bfloat16),
            pltpu.VMEM((chunk // HALVES, half * HALVES), jnp.bfloat16),
            pltpu.VMEM((chunk // HALVES, w_in.shape[1]), jnp.bfloat16),
            pltpu.SemaphoreType.DMA((STEPS,)),
            pltpu.SemaphoreType.DMA((w_in.shape[1] // SPAN,)),
            pltpu.SemaphoreType.DMA((HALVES,)),
        ],
        compiler_params=pltpu.CompilerParams(vmem_limit_bytes=56 << 20),
        name="ffn",
    )(rows, w_in, w_out)


def mixing_kernel(codes_ref, gates_ref, out_ref):
    halves, group, count = out_ref.shape
    here = lax.broadcasted_iota(jnp.int32, (group, count), 1)
    slot = here // BLOCK * SLOTS + here % SLOTS
    side = here // SLOTS % HALVES
    total = jnp.where(slot == codes_ref[:, 0:1], gates_ref[:, 0:1], 0.0)
    total = jnp.where(slot == codes_ref[:, 1:2], gates_ref[:, 1:2], total)
    for h in range(halves):
        out_ref[h] = jnp.where(side == h, total, 0.0).astype(jnp.bfloat16)


def mixing(codes, gates, count):
    vmem = pl.BlockSpec(memory_space=pltpu.VMEM)
    return pl.pallas_call(
        mixing_kernel,
        in_specs=[vmem, vmem],
        out_specs=vmem,
        out_shape=pltpu.HBM((HALVES, codes.shape[0], count), jnp.bfloat16),
        name="mixing",
    )(codes, gates)


def combine_kernel(here_ref, weights_ref, table_ref, *refs):
    *sum_refs, out_hbm, loss_ref, out_ref, out_sem = refs
    half = table_ref.shape[1]
    parts = out_sem.shape[1]
    span = half // parts
    planes = len(sum_refs)
    experts = sum_refs[0].shape[1]

    def store(h, j):
        cols = pl.ds(h * half + j * span, span)
        return pltpu.make_async_copy(out_ref.at[:, cols], out_hbm.at[:, cols], out_sem.at[h, j])

    sums = [ref[...] for ref in sum_refs]
    totals = jnp.zeros_like(sums[0])
    for plane in range(planes):
        for d, value in enumerate(sums):
            mine = (here_ref[0] + d) % planes == plane
            totals += jnp.where(mine, value, 0.0)
    all_tokens = out_hbm.shape[0] * experts
    share = totals / all_tokens
    loss_ref[...] = experts * jnp.sum(share[0:1, :] * share[1:2, :], axis=1, keepdims=True)
    for j in range(parts):
        for h in range(HALVES):
            start = h * half + j * span
            out_ref[:, start : start + span] = jnp.dot(
                weights_ref[h],
                table_ref[:, j * span : (j + 1) * span],
                preferred_element_type=jnp.float32,
            ).astype(jnp.bfloat16)
            store(h, j).start()
    for j in range(parts):
        for h in range(HALVES):
            store(h, j).wait()


def combine(here, weights, table, sums):
    group = weights.shape[1]
    half = table.shape[1]
    hbm = pl.BlockSpec(memory_space=pltpu.HBM)
    vmem = pl.BlockSpec(memory_space=pltpu.VMEM)
    return pl.pallas_call(
        combine_kernel,
        in_specs=[pl.BlockSpec(memory_space=pltpu.SMEM), vmem, vmem] + [vmem] * len(sums),
        out_specs=[hbm, vmem],
        out_shape=[
            pltpu.HBM((group, half * HALVES), jnp.bfloat16),
            jax.ShapeDtypeStruct((1, 1), jnp.float32),
        ],
        scratch_shapes=[
            pltpu.VMEM((group, half * HALVES), jnp.bfloat16),
            pltpu.SemaphoreType.DMA((HALVES, half // SPAN)),
        ],
        compiler_params=pltpu.CompilerParams(vmem_limit_bytes=24 << 20),
        name="combine",
    )(here, weights, table, *sums)


def exchange(rows):
    count, half = rows.shape
    blocks = rows.reshape(count // BLOCK, BLOCK, half)
    blocks = lax.all_to_all(blocks, ROUTE, split_axis=0, concat_axis=0, tiled=True)
    return blocks.reshape(count, half)


def shards(tokens, routes, priority, router, w_in, w_out):
    group = tokens.shape[0]
    experts = router.shape[1]
    sizes = {axis: lax.axis_size(axis) for axis in EXPERT_DP}
    planes = sizes[RING]
    outgoing, codes = dispatch(routes.T, priority, tokens, experts, sizes)
    arrived = exchange(outgoing)

    late, codes, routes, _ = lax.optimization_barrier((tokens, codes, routes, outgoing))
    logits = jnp.dot(late, router, preferred_element_type=jnp.float32)
    probs = jax.nn.softmax(logits, axis=-1)
    expert_grid = lax.broadcasted_iota(jnp.int32, (group, experts), 1)
    first_hot = (expert_grid == routes[:, 0:1]).astype(jnp.float32)
    second_hot = (expert_grid == routes[:, 1:2]).astype(jnp.float32)
    logit_first = jnp.sum(logits * first_hot, axis=1)
    logit_second = jnp.sum(logits * second_hot, axis=1)
    gates = jnp.stack(
        [
            jax.nn.sigmoid(logit_first - logit_second),
            jax.nn.sigmoid(logit_second - logit_first),
        ],
        axis=1,
    )
    gates = gates.astype(jnp.bfloat16).astype(jnp.float32)
    statistics = jnp.stack([jnp.sum(probs, axis=0), jnp.sum(first_hot, axis=0)], axis=0)
    for axis in PLANE:
        statistics = lax.psum(statistics, axis)
    sums = [statistics]
    for d in range(1, planes):
        ring = [(i, (i - d) % planes) for i in range(planes)]
        sums.append(lax.ppermute(statistics, RING, ring))
    mixers = mixing(codes.T, gates, outgoing.shape[0])
    arrived, mixers = lax.optimization_barrier((arrived, mixers))
    produced = expert_ffn(arrived, w_in[0], w_out[0])
    here = lax.axis_index(RING).reshape(1)
    here, produced, *sums = lax.optimization_barrier((here, produced, *sums))
    returned = exchange(produced)
    mixed, loss = combine(here, mixers, returned, sums)
    return mixed, loss[0, 0]


def solution(mesh):
    torus = Mesh(
        mesh.devices.reshape(4, 8, 2, mesh.shape["dp"]), ("expert_0", "expert_1", "expert_2", "dp")
    )
    placed = (
        P(EXPERT_DP, None),
        P(EXPERT_DP, None),
        P(EXPERT_DP, None),
        P(),
        P(EXPERT_DP, None, None),
        P(EXPERT_DP, None, None),
    )

    return jax.shard_map(
        shards, mesh=torus, in_specs=placed, out_specs=(P(EXPERT_DP, None), P()), check_vma=False
    )
```

```python
import functools

import jax
import jax.numpy as jnp
from jax import lax
from jax.experimental import pallas as pl
from jax.experimental.pallas import tpu as pltpu
from jax.sharding import Mesh
from jax.sharding import PartitionSpec as P


EXPERT_DP = ("expert_0", "expert_1", "expert_2", "dp")
ROUTE = ("expert_2", "expert_0", "dp", "expert_1")
PLANE = ("expert_0", "expert_2", "dp")
RING = "expert_1"
SLOTS = 4
HALVES = 2
BLOCK = SLOTS * HALVES
STEPS = 2
DSTEPS = 8
SPAN = 512


def number(expert, sizes):
    planes, cores, columns = sizes["expert_1"], sizes["expert_2"], sizes["dp"]
    y = expert % columns
    core = (expert // columns) % cores
    z = (expert // (columns * cores)) % planes
    x = expert // (columns * cores * planes)
    return ((core * sizes["expert_0"] + x) * columns + y) * planes + z


def dispatch_kernel(
    routes_hbm,
    ranks_hbm,
    tokens_hbm,
    out_hbm,
    codes_ref,
    routes_ref,
    ranks_ref,
    tokens_ref,
    out_ref,
    i_sem,
    t_sem,
    o_sem,
    *,
    sizes,
):
    group, width = tokens_ref.shape
    half = width // HALVES
    steps = o_sem.shape[0]
    chunk = out_ref.shape[0] // steps
    experts = out_ref.shape[0] // BLOCK
    count = chunk // HALVES
    small = [
        pltpu.make_async_copy(routes_hbm, routes_ref, i_sem.at[0]),
        pltpu.make_async_copy(ranks_hbm, ranks_ref, i_sem.at[1]),
    ]
    load = pltpu.make_async_copy(tokens_hbm, tokens_ref, t_sem)
    for copy in (*small, load):
        copy.start()
    for copy in small:
        copy.wait()
    first = routes_ref[0:1, :]
    second = routes_ref[1:2, :]
    ids = lax.broadcasted_iota(jnp.int32, (experts, group), 0)
    first_hot = jnp.where(ids == first, 1.0, 0.0)
    second_hot = jnp.where(ids == second, 1.0, 0.0)
    rows = lax.broadcasted_iota(jnp.int32, (group, group), 0)
    lanes = lax.broadcasted_iota(jnp.int32, (group, group), 1)
    ranks = ranks_ref[...].astype(jnp.float32)
    column = jnp.sum(jnp.where(rows == lanes, ranks, 0.0), axis=1, keepdims=True)
    earlier = jnp.where(column < ranks, 1.0, 0.0).astype(jnp.bfloat16)
    before_first = jnp.dot(
        first_hot.astype(jnp.bfloat16), earlier, preferred_element_type=jnp.float32
    )
    before_second = jnp.dot(
        second_hot.astype(jnp.bfloat16), earlier, preferred_element_type=jnp.float32
    )
    first_load = jnp.sum(first_hot, axis=1, keepdims=True)
    pos_first = jnp.sum(before_first * first_hot, axis=0, keepdims=True).astype(jnp.int32)
    pos_second = jnp.sum((before_second + first_load) * second_hot, axis=0, keepdims=True).astype(
        jnp.int32
    )
    slot_first = jnp.where(pos_first < SLOTS, number(first, sizes) * SLOTS + pos_first, -1)
    slot_second = jnp.where(pos_second < SLOTS, number(second, sizes) * SLOTS + pos_second, -1)
    codes_ref[0:1, :] = slot_first
    codes_ref[1:2, :] = slot_second
    load.wait()
    copies = []
    for i in range(steps):
        here = lax.broadcasted_iota(jnp.int32, (count, group), 0) + i * count
        hot = jnp.where((here == slot_first) | (here == slot_second), 1.0, 0.0)
        hot = hot.astype(jnp.bfloat16)
        span = SPAN
        for j in range(half // span):
            sides = []
            for h in range(HALVES):
                cols = slice(h * half + j * span, h * half + (j + 1) * span)
                side = jnp.dot(hot, tokens_ref[:, cols], preferred_element_type=jnp.float32)
                sides.append(side.reshape(count // SLOTS, 1, SLOTS, span))
            out_ref[i * chunk : (i + 1) * chunk, j * span : (j + 1) * span] = (
                jnp.concatenate(sides, axis=1).reshape(chunk, span).astype(jnp.bfloat16)
            )
        part = pl.ds(i * chunk, chunk)
        copies.append(
            pltpu.make_async_copy(out_ref.at[part, :], out_hbm.at[part, :], o_sem.at[i])
        )
        copies[-1].start()
    for copy in copies:
        copy.wait()


def dispatch(routes, ranks, tokens, experts, sizes):
    group, width = tokens.shape
    rows, half = experts * BLOCK, width // HALVES
    hbm = pl.BlockSpec(memory_space=pltpu.HBM)
    vmem = pl.BlockSpec(memory_space=pltpu.VMEM)
    return pl.pallas_call(
        functools.partial(dispatch_kernel, sizes=sizes),
        in_specs=[hbm, hbm, hbm],
        out_specs=[hbm, vmem],
        out_shape=[
            pltpu.HBM((rows, half), jnp.bfloat16),
            jax.ShapeDtypeStruct((2, group), jnp.int32),
        ],
        scratch_shapes=[
            pltpu.VMEM((2, group), jnp.int32),
            pltpu.VMEM((1, group), jnp.int32),
            pltpu.VMEM((group, width), jnp.bfloat16),
            pltpu.VMEM((rows, half), jnp.bfloat16),
            pltpu.SemaphoreType.DMA((2,)),
            pltpu.SemaphoreType.DMA,
            pltpu.SemaphoreType.DMA((DSTEPS,)),
        ],
        name="dispatch",
    )(in_hbm(routes), in_hbm(ranks), in_hbm(tokens))


def fetch_kernel(w_hbm, out_ref, sem):
    copy = pltpu.make_async_copy(w_hbm.at[:, pl.ds(0, SPAN)], out_ref, sem)
    copy.start()
    copy.wait()


def fetch(weights):
    return pl.pallas_call(
        fetch_kernel,
        in_specs=[pl.BlockSpec(memory_space=pltpu.HBM)],
        out_specs=pl.BlockSpec(memory_space=pltpu.VMEM),
        out_shape=pltpu.VMEM((weights.shape[0], SPAN), weights.dtype),
        scratch_shapes=[pltpu.SemaphoreType.DMA],
        name="fetch",
    )(weights)


def ffn_kernel(
    x_hbm,
    head_ref,
    w_in_hbm,
    w_out_hbm,
    y_ref,
    x_ref,
    w_in_ref,
    w_out_ref,
    sorted_ref,
    hidden_ref,
    x_sem,
    in_sem,
    foot_sem,
):
    half = x_ref.shape[1]
    steps = x_sem.shape[0]
    chunk = x_ref.shape[0] // steps
    blocks = chunk // BLOCK
    count = blocks * SLOTS
    transposed = (((1,), (1,)), ((), ()))

    def x_copy(i):
        rows = pl.ds(i * chunk, chunk)
        return pltpu.make_async_copy(x_hbm.at[rows, :], x_ref.at[rows, :], x_sem.at[i])

    def in_copy(j):
        cols = pl.ds(j * SPAN, SPAN)
        return pltpu.make_async_copy(w_in_hbm.at[:, cols], w_in_ref.at[:, cols], in_sem.at[j - 1])

    def foot_copy(h):
        rows = pl.ds(h * half, half)
        return pltpu.make_async_copy(w_out_hbm.at[rows, :], w_out_ref.at[rows, :], foot_sem.at[h])

    x_copy(0).start()
    spans = w_in_ref.shape[1] // SPAN
    for j in range(1, spans):
        in_copy(j).start()
    for i in range(steps):
        top = i * chunk
        x_copy(i).wait()
        if i == 0:
            for h in range(HALVES):
                foot_copy(h).start()
        if i + 1 < steps:
            x_copy(i + 1).start()
        rows = x_ref[top : top + chunk, :].astype(jnp.float32)
        rows = rows.reshape(blocks, HALVES, SLOTS, half)
        for h in range(HALVES):
            sorted_ref[:, h * half : (h + 1) * half] = (
                rows[:, h].reshape(count, half).astype(jnp.bfloat16)
            )
        for j in range(w_in_ref.shape[1] // SPAN):
            if i == 0 and j > 0:
                in_copy(j).wait()
            cols = slice(j * SPAN, (j + 1) * SPAN)
            part = w_in_ref[:, cols] if j else head_ref[...]
            total = jnp.dot(sorted_ref[...], part, preferred_element_type=jnp.float32)
            hidden_ref[:, cols] = jnp.maximum(total, 0.0).astype(jnp.bfloat16)
        for j in range(half // SPAN):
            sides = []
            for h in range(HALVES):
                if i == 0 and j == 0:
                    foot_copy(h).wait()
                feet = slice(h * half + j * SPAN, h * half + (j + 1) * SPAN)
                side = lax.dot_general(
                    hidden_ref[...],
                    w_out_ref[feet, :],
                    transposed,
                    preferred_element_type=jnp.float32,
                )
                sides.append(side.reshape(blocks, 1, SLOTS, SPAN))
            y_ref[top : top + chunk, j * SPAN : (j + 1) * SPAN] = (
                jnp.concatenate(sides, axis=1).reshape(chunk, SPAN).astype(jnp.bfloat16)
            )


def expert_ffn(rows, head, w_in, w_out):
    count, half = rows.shape
    chunk = count // STEPS
    hbm = pl.BlockSpec(memory_space=pltpu.HBM)
    return pl.pallas_call(
        ffn_kernel,
        in_specs=[hbm, pl.BlockSpec(memory_space=pltpu.VMEM), hbm, hbm],
        out_specs=pl.BlockSpec(memory_space=pltpu.VMEM),
        out_shape=pltpu.VMEM((count, half), jnp.bfloat16),
        scratch_shapes=[
            pltpu.VMEM((count, half), jnp.bfloat16),
            pltpu.VMEM(w_in.shape, jnp.bfloat16),
            pltpu.VMEM(w_out.shape, jnp.bfloat16),
            pltpu.VMEM((chunk // HALVES, half * HALVES), jnp.bfloat16),
            pltpu.VMEM((chunk // HALVES, w_in.shape[1]), jnp.bfloat16),
            pltpu.SemaphoreType.DMA((STEPS,)),
            pltpu.SemaphoreType.DMA((w_in.shape[1] // SPAN - 1,)),
            pltpu.SemaphoreType.DMA((HALVES,)),
        ],
        compiler_params=pltpu.CompilerParams(vmem_limit_bytes=40 << 20),
        name="ffn",
    )(in_hbm(rows), head, in_hbm(w_in), in_hbm(w_out))


def mixing_kernel(codes_ref, gates_ref, out_ref):
    halves, group, count = out_ref.shape
    here = lax.broadcasted_iota(jnp.int32, (group, count), 1)
    slot = here // BLOCK * SLOTS + here % SLOTS
    side = here // SLOTS % HALVES
    total = jnp.where(slot == codes_ref[:, 0:1], gates_ref[:, 0:1], 0.0)
    total = jnp.where(slot == codes_ref[:, 1:2], gates_ref[:, 1:2], total)
    for h in range(halves):
        out_ref[h] = jnp.where(side == h, total, 0.0).astype(jnp.bfloat16)


def mixing(codes, gates, count):
    vmem = pl.BlockSpec(memory_space=pltpu.VMEM)
    return pl.pallas_call(
        mixing_kernel,
        in_specs=[vmem, vmem],
        out_specs=vmem,
        out_shape=pltpu.HBM((HALVES, codes.shape[0], count), jnp.bfloat16),
        name="mixing",
    )(codes, gates)


def combine_kernel(here_ref, weights_ref, table_ref, *refs):
    *sum_refs, out_hbm, loss_ref, out_ref, out_sem = refs
    half = table_ref.shape[1]
    parts = out_sem.shape[1]
    span = half // parts
    planes = len(sum_refs)
    experts = sum_refs[0].shape[1]

    def store(h, j):
        cols = pl.ds(h * half + j * span, span)
        return pltpu.make_async_copy(out_ref.at[:, cols], out_hbm.at[:, cols], out_sem.at[h, j])

    sums = [ref[...] for ref in sum_refs]
    totals = jnp.zeros_like(sums[0])
    for plane in range(planes):
        for d, value in enumerate(sums):
            mine = (here_ref[0] + d) % planes == plane
            totals += jnp.where(mine, value, 0.0)
    all_tokens = out_hbm.shape[0] * experts
    share = totals / all_tokens
    loss_ref[...] = experts * jnp.sum(share[0:1, :] * share[1:2, :], axis=1, keepdims=True)
    for j in range(parts):
        for h in range(HALVES):
            start = h * half + j * span
            out_ref[:, start : start + span] = jnp.dot(
                weights_ref[h],
                table_ref[:, j * span : (j + 1) * span],
                preferred_element_type=jnp.float32,
            ).astype(jnp.bfloat16)
            store(h, j).start()
    for j in range(parts):
        for h in range(HALVES):
            store(h, j).wait()


def combine(here, weights, table, sums):
    group = weights.shape[1]
    half = table.shape[1]
    hbm = pl.BlockSpec(memory_space=pltpu.HBM)
    vmem = pl.BlockSpec(memory_space=pltpu.VMEM)
    return pl.pallas_call(
        combine_kernel,
        in_specs=[pl.BlockSpec(memory_space=pltpu.SMEM), vmem, vmem] + [vmem] * len(sums),
        out_specs=[hbm, vmem],
        out_shape=[
            pltpu.HBM((group, half * HALVES), jnp.bfloat16),
            jax.ShapeDtypeStruct((1, 1), jnp.float32),
        ],
        scratch_shapes=[
            pltpu.VMEM((group, half * HALVES), jnp.bfloat16),
            pltpu.SemaphoreType.DMA((HALVES, half // SPAN)),
        ],
        compiler_params=pltpu.CompilerParams(vmem_limit_bytes=24 << 20),
        name="combine",
    )(here, weights, table, *sums)


def in_hbm(value):
    return pltpu.with_memory_space_constraint(value, pltpu.HBM)


def exchange(rows):
    count, half = rows.shape
    blocks = rows.reshape(count // BLOCK, BLOCK, half)
    blocks = lax.all_to_all(blocks, ROUTE, split_axis=0, concat_axis=0, tiled=True)
    return blocks.reshape(count, half)


def shards(tokens, routes, priority, router, w_in, w_out):
    group = tokens.shape[0]
    experts = router.shape[1]
    sizes = {axis: lax.axis_size(axis) for axis in EXPERT_DP}
    planes = sizes[RING]
    outgoing, codes = dispatch(routes.T, priority, tokens, experts, sizes)
    arrived = exchange(outgoing)

    late, codes, routes, _ = lax.optimization_barrier((tokens, codes, routes, outgoing))
    logits = jnp.dot(late, router, preferred_element_type=jnp.float32)
    probs = jax.nn.softmax(logits, axis=-1)
    expert_grid = lax.broadcasted_iota(jnp.int32, (group, experts), 1)
    first_hot = (expert_grid == routes[:, 0:1]).astype(jnp.float32)
    second_hot = (expert_grid == routes[:, 1:2]).astype(jnp.float32)
    logit_first = jnp.sum(logits * first_hot, axis=1)
    logit_second = jnp.sum(logits * second_hot, axis=1)
    gates = jnp.stack(
        [
            jax.nn.sigmoid(logit_first - logit_second),
            jax.nn.sigmoid(logit_second - logit_first),
        ],
        axis=1,
    )
    gates = gates.astype(jnp.bfloat16).astype(jnp.float32)
    statistics = jnp.stack([jnp.sum(probs, axis=0), jnp.sum(first_hot, axis=0)], axis=0)
    for axis in PLANE:
        statistics = lax.psum(statistics, axis)
    sums = [statistics]
    for d in range(1, planes):
        ring = [(i, (i - d) % planes) for i in range(planes)]
        sums.append(lax.ppermute(statistics, RING, ring))
    mixers = mixing(codes.T, gates, outgoing.shape[0])
    head, _ = lax.optimization_barrier((w_in[0], mixers))
    head = fetch(in_hbm(head))
    arrived, mixers, head = lax.optimization_barrier((arrived, mixers, head))
    produced = expert_ffn(arrived, head, w_in[0], w_out[0])
    here = lax.axis_index(RING).reshape(1)
    here, produced, *sums = lax.optimization_barrier((here, produced, *sums))
    returned = exchange(produced)
    mixed, loss = combine(here, mixers, returned, sums)
    return mixed, loss[0, 0]


def solution(mesh):
    torus = Mesh(
        mesh.devices.reshape(4, 8, 2, mesh.shape["dp"]), ("expert_0", "expert_1", "expert_2", "dp")
    )
    placed = (
        P(EXPERT_DP, None),
        P(EXPERT_DP, None),
        P(EXPERT_DP, None),
        P(),
        P(EXPERT_DP, None, None),
        P(EXPERT_DP, None, None),
    )

    return jax.shard_map(
        shards, mesh=torus, in_specs=placed, out_specs=(P(EXPERT_DP, None), P()), check_vma=False
    )
```
